32 devices in a mesh: rep: 1, dp: 32 (over x, y, z, core).
Axes of the slice: x: 2, y: 2, z: 4, core: 2. Of those that a mesh axis runs over, the one named last changes fastest.
Arguments:
- g_w_gate: bfloat16 [32, 2, 1280, 3072], P(('rep', 'dp'))
- g_w_up: bfloat16 [32, 2, 1280, 3072], P(('rep', 'dp'))
- g_w_down: bfloat16 [32, 2, 3072, 1280], P(('rep', 'dp'))
- w_gate: bfloat16 [2, 1280, 3072], replicated
- w_up: bfloat16 [2, 1280, 3072], replicated
- w_down: bfloat16 [2, 3072, 1280], replicated
- m_w_gate: float32 [2, 1280, 3072], P(None, 'dp')
- m_w_up: float32 [2, 1280, 3072], P(None, 'dp')
- m_w_down: float32 [2, 3072, 1280], P(None, 'dp')
- v_w_gate: float32 [2, 1280, 3072], P(None, 'dp')
- v_w_up: float32 [2, 1280, 3072], P(None, 'dp')
- v_w_down: float32 [2, 3072, 1280], P(None, 'dp')
Outputs:
- output 1: bfloat16 [2, 1280, 3072], P('rep')
- output 2: bfloat16 [2, 1280, 3072], P('rep')
- output 3: bfloat16 [2, 3072, 1280], P('rep')
- output 4: float32 [2, 1280, 3072], P('rep', 'dp')
- output 5: float32 [2, 1280, 3072], P('rep', 'dp')
- output 6: float32 [2, 3072, 1280], P('rep', 'dp')
- output 7: float32 [2, 1280, 3072], P('rep', 'dp')
- output 8: float32 [2, 1280, 3072], P('rep', 'dp')
- output 9: float32 [2, 3072, 1280], P('rep', 'dp')
All inputs are finite; a program needn't handle non-finite values.
Results may differ from the reference program's by a relative error of at most 0.022.
Values are sent between devices in bfloat16 or wider.
A program may use at most 2 GiB of HBM per device.

```python
import jax
import jax.numpy as jnp
from jax import lax

DEVICES = 32
D = 1280
FF = 3072
LAYERS = 2
NAMES = ("w_gate", "w_up", "w_down")
SHAPES = {"w_gate": (LAYERS, D, FF), "w_up": (LAYERS, D, FF), "w_down": (LAYERS, FF, D)}


def setup_inputs(seed: int = 0, part: int = 0) -> dict:
    kz, *keys = jax.random.split(jax.random.key(seed), 1 + 5 * len(NAMES))
    loud = 2.0 ** jax.random.uniform(kz, (), jnp.float32, -1.0, 1.0)
    drawn = {}
    for name, key, both in zip(NAMES, keys[:3], keys[3:6], strict=True):
        own = jax.random.normal(jax.random.fold_in(key, part), (DEVICES, *SHAPES[name]), jnp.float32)
        shared = jax.random.normal(jax.random.fold_in(both, part), SHAPES[name], jnp.float32)
        drawn["g_" + name] = (loud * (0.7 * shared / DEVICES + 0.7 * own * DEVICES**-0.5)).astype(jnp.bfloat16)
    for name, key in zip(NAMES, keys[6:9], strict=True):
        drawn[name] = (jax.random.normal(key, SHAPES[name], jnp.float32) * SHAPES[name][1] ** -0.5).astype(jnp.bfloat16)
    for name, key in zip(NAMES, keys[9:12], strict=True):
        drawn["m_" + name] = loud * 0.5 * jax.random.normal(key, SHAPES[name], jnp.float32)
    for name, key in zip(NAMES, keys[12:15], strict=True):
        drawn["v_" + name] = loud * loud * jax.random.uniform(key, SHAPES[name], jnp.float32, 0.5, 1.5)
    return drawn


def adamw(w, m, v, g):
    m = 0.9 * m + 0.1 * g
    v = 0.95 * v + 0.05 * g * g
    step = m * lax.rsqrt(v + 1e-8) + 0.1 * w
    return (w - 0.02 * step).astype(jnp.bfloat16), m, v


def reference(g_w_gate, g_w_up, g_w_down, w_gate, w_up, w_down, m_w_gate, m_w_up, m_w_down, v_w_gate, v_w_up, v_w_down):
    def total(terms):
        return lax.scan(lambda so_far, term: (so_far + term.astype(jnp.float32), None), jnp.zeros(terms.shape[1:], jnp.float32), terms)[0]

    gradients = [total(terms).astype(jnp.bfloat16).astype(jnp.float32) for terms in (g_w_gate, g_w_up, g_w_down)]
    new = [
        adamw(w.astype(jnp.float32), m, v, g)
        for w, m, v, g in zip((w_gate, w_up, w_down), (m_w_gate, m_w_up, m_w_down), (v_w_gate, v_w_up, v_w_down), gradients, strict=True)
    ]
    return tuple(one[which] for which in range(3) for one in new)
```

```python
import functools

import jax
import jax.numpy as jnp
from jax import lax
from jax.experimental import pallas as pl
from jax.experimental.pallas import tpu as pltpu
from jax.sharding import PartitionSpec as P

TILES = 120
CUT = 60
GROUP = 12
SLOTS = 6
F32, BF16 = jnp.float32, jnp.bfloat16


def tiled(a, lead, rows, columns):
    a = a.reshape(2, *lead, rows // 8, 8, columns // 128, 128)
    return jnp.swapaxes(a, a.ndim - 3, a.ndim - 2).reshape(2, *lead, TILES, 8, 128)


def untiled(a, rows, columns):
    n = a.size // (2 * rows * columns)
    a = a.reshape(2, n, rows // 8, columns // 128, 8, 128)
    return jnp.swapaxes(a, 3, 4).reshape(2, n * rows, columns)


def chunks():
    return [(k, l, o) for k in range(3) for l in range(2) for o in range(0, TILES, CUT)]


def kernel(*refs):
    g, w, m, v = (refs[i : i + 3] for i in (0, 3, 6, 9))
    out, new_m, new_v, r0 = (refs[i : i + 3] for i in (12, 15, 18, 21))
    po, t0, kg, kr, r1, r2, r3, wb, mb, vb = refs[24:34]
    (p0s, p0r, lg, lt, lk, lm, p1s, p1r, zs, zr, p3s, p3r, a3s, a3r, gs, gr, a1s, a1r, a0s, a0r, loc, st) = refs[34:]
    todo = chunks()
    n = len(todo)

    me = lax.axis_index("dp")
    core, z, y, x = me % 2, me // 2 % 4, me // 8 % 2, me // 16
    a, b = x * (1 - core) + y * core, y * (1 - core) + x * core
    sa, sb = 2 - core, 1 + core
    far = z // 2
    turn = 1 - 2 * far
    here = z * turn + 3 * far
    outer, inner = here == 0, here == 1
    partner = me + 1 - 2 * core
    beside_a = ((1 - a) * sa + b * sb) * 8 + z * 2 + core
    beside_b = (a * sa + (1 - b) * sb) * 8 + z * 2 + core
    inward, outward = me + 2 * turn, me - 2 * turn

    def xy(one_a, one_b):
        return one_a * sa + one_b * sb

    def along(t):
        return t * turn + 3 * far

    def remote(src, dst, send, recv, device):
        return pltpu.make_async_remote_copy(
            src_ref=src, dst_ref=dst, send_sem=send, recv_sem=recv, device_id={"dp": device}, device_id_type=pl.DeviceIdType.MESH
        )

    def await_(ref, sem):
        pltpu.make_async_copy(ref, ref, sem).wait()

    def part(c):
        return pl.ds(todo[c][2], CUT)

    def add(dst, *terms):
        @pl.loop(0, CUT // GROUP)
        def _(i):
            at = pl.ds(i * GROUP, GROUP)
            total = terms[0][at].astype(F32)
            for term in terms[1:]:
                total = total + term[at].astype(F32)
            dst[at] = total.astype(BF16)

    def p0(c):
        k, l, _ = todo[c]
        return remote(g[k].at[l, :, :, 1 - core, part(c)], r0[k].at[l, :, :, part(c)], p0s.at[c], p0r.at[c], partner)

    def load_out(c):
        k, l, _ = todo[c]
        return [pltpu.make_async_copy(g[k].at[l, xy(1 - a, j), :, core, part(c)], po.at[c, j], lg.at[c, j]) for j in range(2)]

    def load_out_r0(c):
        k, l, _ = todo[c]
        return [pltpu.make_async_copy(r0[k].at[l, xy(1 - a, j), :, part(c)], t0.at[c % 3, j], lt.at[c % 3, j]) for j in range(2)]

    def load_kept(c):
        k, l, _ = todo[c]
        s = c % SLOTS
        return [pltpu.make_async_copy(g[k].at[l, xy(a, j), :, core, part(c)], kg.at[s, j], lk.at[s, j]) for j in range(2)] + [
            pltpu.make_async_copy(r0[k].at[l, xy(a, j), :, part(c)], kr.at[s, j], lk.at[s, 2 + j]) for j in range(2)
        ]

    def load_state(c):
        k, l, _ = todo[c]
        return [
            pltpu.make_async_copy(w[k].at[l, x * 2 + y, z, core, part(c)], wb.at[c], lm.at[c, 0]),
            pltpu.make_async_copy(m[k].at[l, part(c)], mb.at[c], lm.at[c, 1]),
            pltpu.make_async_copy(v[k].at[l, part(c)], vb.at[c], lm.at[c, 2]),
        ]

    def store_state(c):
        k, l, _ = todo[c]
        return [
            pltpu.make_async_copy(mb.at[c], new_m[k].at[l, part(c)], st.at[c, 0]),
            pltpu.make_async_copy(vb.at[c], new_v[k].at[l, part(c)], st.at[c, 1]),
        ]

    def p1(c):
        return remote(po.at[c], r1.at[c], p1s.at[c], p1r.at[c], beside_a)

    def zsend(c, i, t, slot, device):
        return remote(kg.at[c % SLOTS, :, along(t)], r2.at[c, slot], zs.at[c, i], zr.at[c, slot], device)

    def p3(c):
        return remote(kg.at[c % SLOTS, 1 - b, z], r3.at[c], p3s.at[c], p3r.at[c], beside_b)

    def a3(c):
        return remote(r1.at[c, b, z], r1.at[c, b, z], a3s.at[c], a3r.at[c], beside_b)

    def gsend(c, i, t, slot, device):
        where = r1.at[c, :, along(t)]
        return remote(where, where, gs.at[c, i], gr.at[c, slot], device)

    def spread(c, t):
        k, l, _ = todo[c]
        for j in range(2):
            src, dst = r1.at[c, j, t], out[k].at[l, xy(a, j), t, core, part(c)]
            remote(src, dst, a1s.at[c], a1r.at[c], beside_a).start()
            remote(src, dst, a0s.at[c], a0r.at[c], partner).start()
            pltpu.make_async_copy(src, dst, loc.at[c]).start()

    def relay(c):
        k, l, _ = todo[c]
        for j in range(2):
            where = out[k].at[l, xy(1 - a, j), :, core, part(c)]
            remote(where, where, a0s.at[c], a0r.at[c], partner).start()

    def kept_terms(c, j, t, *slots):
        s = c % SLOTS
        return (kg.at[s, j, t], kr.at[s, j, t], r1.at[c, j, t], *(r2.at[c, i, j] for i in slots))

    def sum_piece(c, t, *slots):
        for j in range(2):
            add(kg.at[c % SLOTS, j, along(t)], *kept_terms(c, j, along(t), *slots))

    freed, ready = set(range(SLOTS)), set()

    def maybe_load(c):
        if c in freed and c in ready:
            for one in load_kept(c):
                one.start()

    def step_l(c):
        await_(r0[todo[c][0]].at[todo[c][1], :, :, part(c)], p0r.at[c])
        for one in load_out_r0(c):
            one.start()
        ready.add(c)
        maybe_load(c)

    def step_e(c):
        for one in load_out(c) + load_out_r0(c):
            one.wait()

        @pl.loop(0, 8)
        def _(i):
            add(po.at[c, i // 4, i % 4], po.at[c, i // 4, i % 4], t0.at[c % 3, i // 4, i % 4])

        p1(c).start()

    def step_z0(c):
        for one in load_kept(c):
            one.wait()
        await_(r1.at[c], p1r.at[c])

        @pl.when(outer)
        def _():
            for i, t in enumerate((3, 2, 1)):
                sum_piece(c, t)
                zsend(c, i, t, i, inward).start()

    def step_z1(c):
        @pl.when(inner)
        def _():
            await_(r2.at[c, 0], zr.at[c, 0])
            sum_piece(c, 3, 0)
            zsend(c, 0, 3, 3, inward).start()

    def step_z2(c):
        @pl.when(inner)
        def _():
            await_(r2.at[c, 1], zr.at[c, 1])
            sum_piece(c, 2, 1)
            zsend(c, 1, 2, 4, inward).start()

    def step_z3(c):
        @pl.when(inner)
        def _():
            await_(r2.at[c, 3], zr.at[c, 3])
            sum_piece(c, 0, 3)
            zsend(c, 2, 0, 3, outward).start()

    def step_f(c):
        @pl.when(outer)
        def _():
            await_(r2.at[c, 3], zr.at[c, 3])
            add(kg.at[c % SLOTS, 1 - b, z], *kept_terms(c, 1 - b, z, 3))

        @pl.when(inner)
        def _():
            await_(r2.at[c, 2], zr.at[c, 2])
            await_(r2.at[c, 4], zr.at[c, 4])
            add(kg.at[c % SLOTS, 1 - b, z], *kept_terms(c, 1 - b, z, 2, 4))

        p3(c).start()

    def step_g(c):
        await_(r3.at[c], p3r.at[c])
        gradient = kg.at[c % SLOTS, b, z]

        @pl.when(outer)
        def _():
            add(gradient, *kept_terms(c, b, z, 3), r3.at[c])

        @pl.when(inner)
        def _():
            add(gradient, *kept_terms(c, b, z, 2, 4), r3.at[c])

        for one in load_state(c):
            one.wait()

        @pl.loop(0, CUT // GROUP)
        def _(i):
            at = pl.ds(i * GROUP, GROUP)
            grad = gradient[at].astype(F32)
            one_m = 0.9 * mb[c, at] + 0.1 * grad
            one_v = 0.95 * vb[c, at] + 0.05 * grad * grad
            one_w = wb[c, at].astype(F32)
            mb[c, at] = one_m
            vb[c, at] = one_v
            r1[c, b, z, at] = (one_w - 0.02 * (one_m * lax.rsqrt(one_v + 1e-8) + 0.1 * one_w)).astype(BF16)

        a3(c).start()
        for one in store_state(c):
            one.start()

    def step_h(c):
        await_(r1.at[c, 1 - b, z], a3r.at[c])

        @pl.when(outer)
        def _():
            gsend(c, 0, 0, 0, inward).start()

        @pl.when(inner)
        def _():
            gsend(c, 0, 1, 0, outward).start()
            gsend(c, 1, 1, 1, inward).start()

        spread(c, z)

    def step_r(c):
        for i in range(3):
            await_(kg.at[c % SLOTS, :, 0], zs.at[c, i])
        await_(r3.at[c], p3s.at[c])
        freed.add(c + SLOTS)
        maybe_load(c + SLOTS)

    def step_i(c, i):
        @pl.when(outer)
        def _():
            await_(r1.at[c, :, along(i + 1)], gr.at[c, i])
            spread(c, along(i + 1))

        @pl.when(inner)
        def _():
            t = (0, 2, 3)[i]
            await_(r1.at[c, :, along(t)], gr.at[c, i])
            if i == 0:
                gsend(c, 2, 0, 2, inward).start()
            else:
                gsend(c, 2 + i, t, i, outward).start()
            spread(c, along(t))

    def step_k(c):
        await_(r1.at[c], a1r.at[c])
        relay(c)

    unit = CUT / 60
    events = []
    for c in range(n):
        first = (18 + 16 * c) * unit
        events.append(((5 + 4 * (c - 1)) * unit, step_l, (c,)))
        events.append(((6 + 4 * c) * unit, step_e, (c,)))
        events.append((first, step_z0, (c,)))
        events.append((first + 8 * unit, step_z1, (c,)))
        events.append((first + 14 * unit, step_z2, (c,)))
        events.append((first + 14.1 * unit, step_z3, (c,)))
        events.append((first + 21 * unit, step_f, (c,)))
        events.append((first + 25 * unit, step_g, (c,)))
        events.append((first + 29 * unit, step_h, (c,)))
        events.append((first + 31 * unit, step_r, (c,)))
        for i in range(3):
            events.append((first + (37 + 7 * i) * unit, step_i, (c, i)))
        events.append((first + 66 * unit, step_k, (c,)))
    events.sort(key=lambda one: one[0])

    for c in range(n):
        p0(c).start()
        for one in load_out(c):
            one.start()
    for c in range(n):
        for one in load_state(c):
            one.start()
    for _, step, args in events:
        step(*args)

    for c, (k, l, _) in enumerate(todo):
        await_(out[k].at[l, :, :, 1 - core, part(c)], a0r.at[c])
        await_(r0[k].at[l, :, :, part(c)], p0s.at[c])
        await_(out[k].at[l, :, :, 1 - core, part(c)], a0s.at[c])
        await_(r1.at[c], p1s.at[c])
        await_(r1.at[c], a1s.at[c])
        await_(r1.at[c], loc.at[c])
        await_(r3.at[c], a3s.at[c])
        for one in store_state(c):
            one.wait()

        @pl.when(outer)
        def _():
            await_(r1.at[c, :, 0], gs.at[c, 0])

        @pl.when(inner)
        def _():
            for i in range(5):
                await_(r1.at[c, :, 0], gs.at[c, i])


def solution(mesh):
    shapes = ((40, 3072), (40, 3072), (96, 1280))
    n = len(chunks())
    any_ = pl.BlockSpec(memory_space=pl.ANY)

    def step(*arrays):
        g, w, m, v = (arrays[i : i + 3] for i in (0, 3, 6, 9))
        g = [tiled(one[0], (4, 4, 2), *s) for one, s in zip(g, shapes, strict=True)]
        w = [tiled(one, (4, 4, 2), *s) for one, s in zip(w, shapes, strict=True)]
        m = [tiled(one, (), *s) for one, s in zip(m, shapes, strict=True)]
        v = [tiled(one, (), *s) for one, s in zip(v, shapes, strict=True)]
        dma = lambda *shape: pltpu.SemaphoreType.DMA(shape)
        vmem = lambda *shape, dtype=BF16: pltpu.VMEM((*shape, 8, 128), dtype)
        new = pl.pallas_call(
            kernel,
            out_shape=[jax.ShapeDtypeStruct((2, 4, 4, 2, TILES, 8, 128), BF16)] * 3
            + [jax.ShapeDtypeStruct((2, TILES, 8, 128), F32)] * 6
            + [jax.ShapeDtypeStruct((2, 4, 4, TILES, 8, 128), BF16)] * 3,
            in_specs=[any_] * 12,
            out_specs=[any_] * 12,
            scratch_shapes=[
                vmem(n, 2, 4, CUT),
                vmem(3, 2, 4, CUT),
                vmem(SLOTS, 2, 4, CUT),
                vmem(SLOTS, 2, 4, CUT),
                vmem(n, 2, 4, CUT),
                vmem(n, 5, 2, CUT),
                vmem(n, CUT),
                vmem(n, CUT),
                vmem(n, CUT, dtype=F32),
                vmem(n, CUT, dtype=F32),
                dma(n),
                dma(n),
                dma(n, 2),
                dma(3, 2),
                dma(SLOTS, 4),
                dma(n, 3),
                dma(n),
                dma(n),
                dma(n, 3),
                dma(n, 5),
                dma(n),
                dma(n),
                dma(n),
                dma(n),
                dma(n, 5),
                dma(n, 3),
                dma(n),
                dma(n),
                dma(n),
                dma(n),
                dma(n),
                dma(n, 2),
            ],
            compiler_params=pltpu.CompilerParams(has_side_effects=True, vmem_limit_bytes=67_043_328),
        )(*g, *w, *m, *v)
        shape_of = lambda i: shapes[i % 3]
        return tuple(untiled(one, *shape_of(i)) for i, one in enumerate(new[:9]))

    all_of, cut = P(None, None, None), P(None, "dp", None)
    return jax.shard_map(
        step,
        mesh=mesh,
        in_specs=(P(("rep", "dp"), None, None, None),) * 3 + (all_of,) * 3 + (cut,) * 6,
        out_specs=(P("rep", None, None),) * 3 + (P("rep", "dp", None),) * 6,
        check_vma=False,
    )
```

```python
import functools

import jax
import jax.numpy as jnp
from jax import lax
from jax.experimental import pallas as pl
from jax.experimental.pallas import tpu as pltpu
from jax.sharding import PartitionSpec as P

TILES = 120
CUT = 60
GROUP = 12
SLOTS = 6
HOLD = 5
LIMIT_A, LIMIT_B = 31 << 20, 31 << 20
F32, BF16 = jnp.float32, jnp.bfloat16


def tiled(a, lead, rows, columns):
    a = a.reshape(2, *lead, rows // 8, 8, columns // 128, 128)
    return jnp.swapaxes(a, a.ndim - 3, a.ndim - 2).reshape(2, *lead, TILES, 8, 128)


def untiled(a, rows, columns):
    n = a.size // (2 * rows * columns)
    a = a.reshape(2, n, rows // 8, columns // 128, 8, 128)
    return jnp.swapaxes(a, 3, 4).reshape(2, n * rows, columns)


def chunks():
    return [(k, l, o) for k in range(3) for l in range(2) for o in range(0, TILES, CUT)]


def plan(n):
    tile = 2048e-3
    hop, z_rate, x_rate, b_rate, pair_rate = 1.5, 46.6e3, 90e3, 46e3, 600e3
    rank = dict(z1=0, z2=0, z3=0, z0=1, f=2, g=3, e=4, l=4, h=5, q=5.5, i=6, r=7, k=8)
    free, arrived, sent, now = {}, {}, {}, [0.0, 0.0]
    done = [{}, {}]
    pair = 4.0
    for c in range(n):
        pair += 16 * CUT * tile / pair_rate * 1e3
        arrived[0, "p0", c] = arrived[1, "p0", c] = pair + hop

    def send(p, link, blocks, rate, at, to, *name):
        start = max(at + 0.3, free.get((p, link), 0.0))
        end = start + blocks * CUT * tile / rate * 1e3 + (0.4 if link == "x" else 0.0)
        free[p, link] = end
        arrived[(to, *name)] = end + hop
        sent[(p, link, *name)] = end + hop

    def after(p, name, c, i=0):
        past = lambda *one, plus=0.0: None if one not in done[p] else done[p][one] + plus
        come = lambda *one: arrived.get((p, *one))
        if name == "l":
            return [come("p0", c)] + ([past("l", c - 1)] if c else []) + ([past("e", c - 3)] if c >= 3 else [])
        if name == "e":
            return [past("l", c, plus=1.5)]
        if name == "z0":
            return [come("p1", c), past("l", c, plus=1.5)] + ([past("r", c - SLOTS, plus=1.5)] if c >= SLOTS else [])
        if name in ("z1", "z2", "z3"):
            return [past("z0", c), come("s" + str((0, 1, 3)[int(name[1]) - 1]), c)]
        if name == "f":
            if p == 0:
                return [past("z0", c), come("s3", c)]
            return [past("z1", c), past("z2", c), past("z3", c), come("s2", c), come("s4", c)]
        if name == "g":
            return [past("f", c), come("p3", c)]
        if name == "h":
            return [past("g", c), come("a3", c)]
        if name == "q":
            return [past("h", c)] + ([past("z0", min(n - 1, c + HOLD))] if p == 0 else [])
        if name == "r":
            if p == 0:
                sends = [sent.get((p, "in", "s" + str(j), c)) for j in range(3)]
            else:
                sends = [sent.get((p, *one, c)) for one in (("in", "s3"), ("in", "s4"), ("out", "s3"))]
            return [past("g", c), sent.get((p, "b", "p3", c)), *sends]
        if name == "i":
            return [past("q", c), come("n" + str(i), c)] + ([past("i", c, i - 1)] if i else [])
        return [past("i", c, 2), come("a1", c)]

    def run(p, at, name, c, i=0):
        work = CUT * 0.004
        if name == "e":
            at += 6 * work + 0.3
            send(p, "x", 8, x_rate, at, p, "p1", c)
        elif name == "z0" and p == 0:
            for j in range(3):
                at += 2 * work + 0.1
                send(p, "in", 2, z_rate, at, 1, "s" + str(j), c)
        elif name in ("z1", "z2"):
            at += 2 * work + 0.1
            send(p, "in", 2, z_rate, at, 1, "s3" if name == "z1" else "s4", c)
        elif name == "z3":
            at += 2 * work + 0.1
            send(p, "out", 2, z_rate, at, 0, "s3", c)
        elif name == "f":
            at += 1.3 * work + 0.1
            send(p, "b", 1, b_rate, at, p, "p3", c)
        elif name == "g":
            at += 4 * work + 0.2
            send(p, "b", 1, b_rate, at, p, "a3", c)
        elif name == "q":
            at += 0.1
            if p == 0:
                send(p, "in", 2, z_rate, at, 1, "n0", c)
            else:
                send(p, "out", 2, z_rate, at, 0, "n0", c)
                send(p, "in", 2, z_rate, at, 1, "n1", c)
        elif name == "i":
            at += 0.3
            if p == 1 and i == 0:
                send(p, "in", 2, z_rate, at, 1, "n2", c)
            elif p == 1:
                send(p, "out", 2, z_rate, at, 0, "n" + str(i), c)
            if i != 1:
                send(p, "x", 4, x_rate, at, p, "a1" if i else "a1 first", c)
        else:
            at += 0.3
        return at

    both = ("l", "e", "z0", "f", "g", "h", "q", "r", "k")
    left = [[(name, c) for c in range(n) for name in both] + [("i", c, i) for c in range(n) for i in range(3)] for _ in range(2)]
    left[1] += [(name, c) for c in range(n) for name in ("z1", "z2", "z3")]
    order = [[], []]
    while left[0] or left[1]:
        best = None
        for p in range(2):
            for one in left[p]:
                times = after(p, *one)
                if None not in times:
                    key = (max(now[p], *times), rank[one[0]], one[1], p, one)
                    best = key if best is None or key < best else best
        at, _, _, p, one = best
        left[p].remove(one)
        now[p] = done[p][one] = run(p, at, *one)
        order[p].append(one)
    return order


def kernel(*refs):
    g, w, m, v = (refs[i : i + 3] for i in (0, 3, 6, 9))
    out, r0, (r1, po, mb, vb) = refs[12:15], refs[15:18], refs[18:22]
    t0, kg, kr, r2, r3, wb = refs[22:28]
    (p0s, p0r, lg, lt, lk, lm, p1s, p1r, zs, zr, p3s, p3r, a3s, a3r, gs, gr, a1s, a1r, a0s, a0r, credit) = refs[28:]
    todo = chunks()
    n = len(todo)

    me = lax.axis_index("dp")
    core, z, y, x = me % 2, me // 2 % 4, me // 8 % 2, me // 16
    a, b = x * (1 - core) + y * core, y * (1 - core) + x * core
    sa, sb = 2 - core, 1 + core
    far = z // 2
    turn = 1 - 2 * far
    here = z * turn + 3 * far
    partner = me + 1 - 2 * core
    beside_a = ((1 - a) * sa + b * sb) * 8 + z * 2 + core
    beside_b = (a * sa + (1 - b) * sb) * 8 + z * 2 + core
    inward, outward = me + 2 * turn, me - 2 * turn

    def xy(one_a, one_b):
        return one_a * sa + one_b * sb

    def along(t):
        return t * turn + 3 * far

    def remote(src, dst, send, recv, device):
        return pltpu.make_async_remote_copy(
            src_ref=src, dst_ref=dst, send_sem=send, recv_sem=recv, device_id={"dp": device}, device_id_type=pl.DeviceIdType.MESH
        )

    def await_(ref, sem):
        pltpu.make_async_copy(ref, ref, sem).wait()

    def part(c):
        return pl.ds(todo[c][2], CUT)

    def add(dst, *terms):
        @pl.loop(0, CUT // GROUP)
        def _(i):
            at = pl.ds(i * GROUP, GROUP)
            total = terms[0][at].astype(F32)
            for term in terms[1:]:
                total = total + term[at].astype(F32)
            dst[at] = total.astype(BF16)

    def p0(c):
        k, l, _ = todo[c]
        return remote(g[k].at[l, :, :, 1 - core, part(c)], r0[k].at[l, :, :, part(c)], p0s.at[c], p0r.at[c], partner)

    def load_out(c):
        k, l, _ = todo[c]
        return [pltpu.make_async_copy(g[k].at[l, xy(1 - a, j), :, core, part(c)], po.at[c, j], lg.at[c, j]) for j in range(2)]

    def load_out_r0(c):
        k, l, _ = todo[c]
        return [pltpu.make_async_copy(r0[k].at[l, xy(1 - a, j), :, part(c)], t0.at[c % 3, j], lt.at[c % 3, j]) for j in range(2)]

    def load_kept(c):
        k, l, _ = todo[c]
        s = c % SLOTS
        return [pltpu.make_async_copy(g[k].at[l, xy(a, j), :, core, part(c)], kg.at[s, j], lk.at[s, j]) for j in range(2)] + [
            pltpu.make_async_copy(r0[k].at[l, xy(a, j), :, part(c)], kr.at[s, j], lk.at[s, 2 + j]) for j in range(2)
        ]

    def load_state(c):
        k, l, _ = todo[c]
        return [
            pltpu.make_async_copy(w[k].at[l, x * 2 + y, z, core, part(c)], wb.at[c], lm.at[c, 0]),
            pltpu.make_async_copy(m[k].at[l, part(c)], mb.at[c], lm.at[c, 1]),
            pltpu.make_async_copy(v[k].at[l, part(c)], vb.at[c], lm.at[c, 2]),
        ]

    def p1(c):
        return remote(po.at[c], r1.at[c], p1s.at[c], p1r.at[c], beside_a)

    def zsend(c, i, t, slot, device):
        return remote(kg.at[c % SLOTS, :, along(t)], r2.at[c, slot], zs.at[c, i], zr.at[c, slot], device)

    def p3(c):
        return remote(kg.at[c % SLOTS, 1 - b, z], r3.at[c], p3s.at[c], p3r.at[c], beside_b)

    def a3(c):
        return remote(r1.at[c, b, z], r1.at[c, b, z], a3s.at[c], a3r.at[c], beside_b)

    def gsend(c, i, t, slot, device):
        where = r1.at[c, :, along(t)]
        return remote(where, where, gs.at[c, i], gr.at[c, slot], device)

    def a1(c, half):
        at = pl.ds(2 * far + 2 * half * turn, 2)
        return remote(r1.at[c, :, at], po.at[c, :, at], a1s.at[c, half], a1r.at[c, half], beside_a)

    def a0(c, mine):
        k, l, _ = todo[c]
        src = r1 if mine else po
        return [
            remote(src.at[c, j], out[k].at[l, xy(a if mine else 1 - a, j), :, part(c)], a0s.at[c], a0r.at[c], partner) for j in range(2)
        ]

    def kept_terms(c, j, t, *slots):
        s = c % SLOTS
        return (kg.at[s, j, t], kr.at[s, j, t], r1.at[c, j, t], *(r2.at[c, i, j] for i in slots))

    def sum_piece(c, t, *slots):
        for j in range(2):
            add(kg.at[c % SLOTS, j, along(t)], *kept_terms(c, j, along(t), *slots))

    def steps(end):
        freed, ready = set(range(SLOTS)), set()

        def maybe_load(c):
            if c in freed and c in ready:
                for one in load_kept(c):
                    one.start()

        last = (3,) if end else (2, 4)

        def step_l(c):
            await_(r0[todo[c][0]].at[todo[c][1], :, :, part(c)], p0r.at[c])
            for one in load_out_r0(c):
                one.start()
            ready.add(c)
            maybe_load(c)

        def step_e(c):
            for one in load_out(c) + load_out_r0(c):
                one.wait()

            @pl.loop(0, 8)
            def _(i):
                add(po.at[c, i // 4, i % 4], po.at[c, i // 4, i % 4], t0.at[c % 3, i // 4, i % 4])

            p1(c).start()

        def step_z0(c):
            for one in load_kept(c):
                one.wait()
            await_(r1.at[c], p1r.at[c])
            await_(po.at[c], p1s.at[c])
            pl.semaphore_signal(credit.at[c], inc=1, device_id={"dp": beside_a}, device_id_type=pl.DeviceIdType.MESH)
            if end:
                for i, t in enumerate((3, 2, 1)):
                    sum_piece(c, t)
                    zsend(c, i, t, i, inward).start()

        def step_z1(c):
            await_(r2.at[c, 0], zr.at[c, 0])
            sum_piece(c, 3, 0)
            zsend(c, 0, 3, 3, inward).start()

        def step_z2(c):
            await_(r2.at[c, 1], zr.at[c, 1])
            sum_piece(c, 2, 1)
            zsend(c, 1, 2, 4, inward).start()

        def step_z3(c):
            await_(r2.at[c, 3], zr.at[c, 3])
            sum_piece(c, 0, 3)
            zsend(c, 2, 0, 3, outward).start()

        def step_f(c):
            for i in last:
                await_(r2.at[c, i], zr.at[c, i])
            add(kg.at[c % SLOTS, 1 - b, z], *kept_terms(c, 1 - b, z, *last))
            p3(c).start()

        def step_g(c):
            await_(r3.at[c], p3r.at[c])
            for one in load_state(c):
                one.wait()
            terms = (*kept_terms(c, b, z, *last), r3.at[c])

            @pl.loop(0, CUT // GROUP)
            def _(i):
                at = pl.ds(i * GROUP, GROUP)
                total = terms[0][at].astype(F32)
                for term in terms[1:]:
                    total = total + term[at].astype(F32)
                grad = total.astype(BF16).astype(F32)
                one_m = 0.9 * mb[c, at] + 0.1 * grad
                one_v = 0.95 * vb[c, at] + 0.05 * grad * grad
                one_w = wb[c, at].astype(F32)
                mb[c, at] = one_m
                vb[c, at] = one_v
                r1[c, b, z, at] = (one_w - 0.02 * (one_m * lax.rsqrt(one_v + 1e-8) + 0.1 * one_w)).astype(BF16)

            a3(c).start()

        def step_h(c):
            await_(r1.at[c, 1 - b, z], a3r.at[c])

        def step_q(c):
            if end:
                gsend(c, 0, 0, 0, inward).start()
            else:
                gsend(c, 0, 1, 0, outward).start()
                gsend(c, 1, 1, 1, inward).start()

        def step_r(c):
            for i in range(3):
                await_(kg.at[c % SLOTS, :, 0], zs.at[c, i])
            await_(r3.at[c], p3s.at[c])
            freed.add(c + SLOTS)
            maybe_load(c + SLOTS)

        def step_i(c, i):
            t = i + 1 if end else (0, 2, 3)[i]
            await_(r1.at[c, :, along(t)], gr.at[c, i])
            if not end and i == 0:
                gsend(c, 2, 0, 2, inward).start()
            elif not end:
                gsend(c, 2 + i, t, i, outward).start()
            if i == 0:
                pl.semaphore_wait(credit.at[c], 1)
                a1(c, 0).start()
            elif i == 2:
                a1(c, 1).start()
                for one in a0(c, True):
                    one.start()

        def step_k(c):
            for half in range(2):
                await_(r1.at[c, :, :2], a1r.at[c, half])
            for one in a0(c, False):
                one.start()

        return dict(
            l=step_l, e=step_e, z0=step_z0, z1=step_z1, z2=step_z2, z3=step_z3, f=step_f,
            g=step_g, h=step_h, q=step_q, r=step_r, i=step_i, k=step_k,
        )

    for c in range(n):
        p0(c).start()
        for one in load_out(c):
            one.start()
    for c in range(n):
        for one in load_state(c):
            one.start()

    order = plan(n)

    @pl.when(here == 0)
    def _():
        take = steps(True)
        for name, *args in order[0]:
            take[name](*args)
        for c in range(n):
            await_(r1.at[c, :, 0], gs.at[c, 0])

    @pl.when(here == 1)
    def _():
        take = steps(False)
        for name, *args in order[1]:
            take[name](*args)
        for c in range(n):
            for i in range(5):
                await_(r1.at[c, :, 0], gs.at[c, i])

    for c, (k, l, _) in enumerate(todo):
        await_(out[k].at[l, :, :, part(c)], a0r.at[c])
        await_(out[k].at[l, :, :, part(c)], a0s.at[c])
        await_(r0[k].at[l, :, :, part(c)], p0s.at[c])
        for half in range(2):
            await_(r1.at[c, :, :2], a1s.at[c, half])
        await_(r3.at[c], a3s.at[c])


def finish(*refs):
    r1, po, mb, vb, *other = refs[:7]
    new_w, new_m, new_v = (refs[i : i + 3] for i in (7, 10, 13))
    buf, here, there, state, ls, ss = refs[16:]
    todo = chunks()
    me = lax.axis_index("dp")
    core, y, x = me % 2, me // 8 % 2, me // 16
    a = x * (1 - core) + y * core
    sa, sb = 2 - core, 1 + core
    copies = []

    def load(c):
        k, l, o = todo[c]
        return pltpu.make_async_copy(other[k].at[l, :, :, pl.ds(o, CUT)], buf.at[c], ls.at[c])

    for c in range(len(todo)):
        load(c).start()
    for c, (k, l, o) in enumerate(todo):
        at = pl.ds(o, CUT)
        for j in range(2):
            copies.append(pltpu.make_async_copy(r1.at[c, j], new_w[k].at[l, a * sa + j * sb, :, core, at], here.at[c, j]))
            copies.append(pltpu.make_async_copy(po.at[c, j], new_w[k].at[l, (1 - a) * sa + j * sb, :, core, at], there.at[c, j]))
        copies.append(pltpu.make_async_copy(mb.at[c], new_m[k].at[l, at], state.at[c, 0]))
        copies.append(pltpu.make_async_copy(vb.at[c], new_v[k].at[l, at], state.at[c, 1]))
    for one in copies:
        one.start()
    for c, (k, l, o) in enumerate(todo):
        load(c).wait()
        one = pltpu.make_async_copy(buf.at[c], new_w[k].at[l, :, :, 1 - core, pl.ds(o, CUT)], ss.at[c])
        one.start()
        copies.append(one)
    for one in copies:
        one.wait()


def solution(mesh):
    shapes = ((40, 3072), (40, 3072), (96, 1280))
    n = len(chunks())
    any_ = pl.BlockSpec(memory_space=pl.ANY)

    def step(*arrays):
        g, w, m, v = (arrays[i : i + 3] for i in (0, 3, 6, 9))
        g = [tiled(one[0], (4, 4, 2), *s) for one, s in zip(g, shapes, strict=True)]
        w = [tiled(one, (4, 4, 2), *s) for one, s in zip(w, shapes, strict=True)]
        m = [tiled(one, (), *s) for one, s in zip(m, shapes, strict=True)]
        v = [tiled(one, (), *s) for one, s in zip(v, shapes, strict=True)]
        dma = lambda *shape: pltpu.SemaphoreType.DMA(shape)
        vmem = lambda *shape, dtype=BF16: pltpu.VMEM((*shape, 8, 128), dtype)
        shape = lambda *shape, dtype=BF16: jax.ShapeDtypeStruct((*shape, 8, 128), dtype)
        on_chip, off_chip = pl.BlockSpec(memory_space=pltpu.VMEM), pl.BlockSpec(memory_space=pltpu.HBM)
        keep = pltpu.with_memory_space_constraint
        *other, _, _, _, r1, po, mb, vb = pl.pallas_call(
            kernel,
            out_shape=[pltpu.HBM((2, 4, 4, TILES, 8, 128), BF16)] * 6 + [vmem(n, 2, 4, CUT)] * 2 + [vmem(n, CUT, dtype=F32)] * 2,
            in_specs=[any_] * 12,
            out_specs=[off_chip] * 6 + [on_chip] * 4,
            scratch_shapes=[
                vmem(3, 2, 4, CUT),
                vmem(SLOTS, 2, 4, CUT),
                vmem(SLOTS, 2, 4, CUT),
                vmem(n, 5, 2, CUT),
                vmem(n, CUT),
                vmem(n, CUT),
                dma(n),
                dma(n),
                dma(n, 2),
                dma(3, 2),
                dma(SLOTS, 4),
                dma(n, 3),
                dma(n),
                dma(n),
                dma(n, 3),
                dma(n, 5),
                dma(n),
                dma(n),
                dma(n),
                dma(n),
                dma(n, 5),
                dma(n, 3),
                dma(n, 2),
                dma(n, 2),
                dma(n),
                dma(n),
                pltpu.SemaphoreType.REGULAR((n,)),
            ],
            compiler_params=pltpu.CompilerParams(has_side_effects=True, vmem_limit_bytes=LIMIT_A),
        )(*g, *w, *m, *v)
        new = pl.pallas_call(
            finish,
            out_shape=[shape(2, 4, 4, 2, TILES)] * 3 + [shape(2, TILES, dtype=F32)] * 6,
            in_specs=[on_chip] * 4 + [off_chip] * 3,
            out_specs=[any_] * 9,
            scratch_shapes=[vmem(n, 4, 4, CUT), dma(n, 2), dma(n, 2), dma(n, 2), dma(n), dma(n)],
            compiler_params=pltpu.CompilerParams(vmem_limit_bytes=LIMIT_B),
        )(*(keep(one, pltpu.VMEM) for one in (r1, po, mb, vb)), *(keep(one, pltpu.HBM) for one in other))
        shape_of = lambda i: shapes[i % 3]
        return tuple(untiled(one, *shape_of(i)) for i, one in enumerate(new))

    all_of, cut = P(None, None, None), P(None, "dp", None)
    return jax.shard_map(
        step,
        mesh=mesh,
        in_specs=(P(("rep", "dp"), None, None, None),) * 3 + (all_of,) * 3 + (cut,) * 6,
        out_specs=(P("rep", None, None),) * 3 + (P("rep", "dp", None),) * 6,
        check_vma=False,
    )
```

```python
import functools

import jax
import jax.numpy as jnp
from jax import lax
from jax.experimental import pallas as pl
from jax.experimental.pallas import tpu as pltpu
from jax.sharding import PartitionSpec as P

TILES = 120
CUT = 40
GROUP = 20
SLOTS = 9
HOLD = 6
LIMIT = 9 << 20
F32, BF16 = jnp.float32, jnp.bfloat16


def tiled(a, lead, rows, columns):
    a = a.reshape(2, *lead, rows // 8, 8, columns // 128, 128)
    return jnp.swapaxes(a, a.ndim - 3, a.ndim - 2).reshape(2, *lead, TILES, 8, 128)


def untiled(a, rows, columns):
    n = a.size // (2 * rows * columns)
    a = a.reshape(2, n, rows // 8, columns // 128, 8, 128)
    return jnp.swapaxes(a, 3, 4).reshape(2, n * rows, columns)


def chunks():
    return [(k, l, o) for k in range(3) for l in range(2) for o in range(0, TILES, CUT)]


def plan(n):
    tile = 2048e-3
    hop, z_rate, x_rate, b_rate, pair_rate = 1.5, 46.6e3, 90e3, 46e3, 600e3
    rank = dict(z1=0, z2=0, z3=0, z0=1, f=2, g=3, e=4, l=4, h=5, q=5.5, i=6, r=7, k=8, w=9)
    free, arrived, sent, now = {}, {}, {}, [0.0, 0.0]
    done = [{}, {}]
    pair = 4.0
    for c in range(n):
        pair += 16 * CUT * tile / pair_rate * 1e3
        arrived[0, "p0", c] = arrived[1, "p0", c] = pair + hop

    def send(p, link, blocks, rate, at, to, *name):
        start = max(at + 0.3, free.get((p, link), 0.0))
        end = start + blocks * CUT * tile / rate * 1e3 + (0.4 if link == "x" else 0.0)
        free[p, link] = end
        arrived[(to, *name)] = end + hop
        sent[(p, link, *name)] = end + hop

    def after(p, name, c, i=0):
        past = lambda *one, plus=0.0: None if one not in done[p] else done[p][one] + plus
        come = lambda *one: arrived.get((p, *one))
        if name == "l":
            return [come("p0", c)] + ([past("l", c - 1)] if c else []) + ([past("e", c - 3)] if c >= 3 else [])
        if name == "e":
            return [past("l", c, plus=1.5)]
        if name == "z0":
            return [come("p1", c), past("l", c, plus=1.5)] + ([past("r", c - SLOTS, plus=1.5)] if c >= SLOTS else [])
        if name in ("z1", "z2", "z3"):
            return [past("z0", c), come("s" + str((0, 1, 3)[int(name[1]) - 1]), c)]
        if name == "f":
            if p == 0:
                return [past("z0", c), come("s3", c)]
            return [past("z1", c), past("z2", c), past("z3", c), come("s2", c), come("s4", c)]
        if name == "g":
            return [past("f", c), come("p3", c)]
        if name == "h":
            return [past("g", c), come("a3", c)]
        if name == "q":
            return [past("h", c)] + ([past("z0", min(n - 1, c + HOLD))] if p == 0 else [])
        if name == "r":
            if p == 0:
                sends = [sent.get((p, "in", "s" + str(j), c)) for j in range(3)]
            else:
                sends = [sent.get((p, *one, c)) for one in (("in", "s3"), ("in", "s4"), ("out", "s3"))]
            return [past("g", c), sent.get((p, "b", "p3", c)), *sends]
        if name == "i":
            return [past("q", c), come("n" + str(i), c)] + ([past("i", c, i - 1)] if i else [])
        if name == "k":
            return [past("i", c, 2), come("a1", c)]
        return [past("k", c), come("a0", c)] + [past("r", j) for j in range(n)]

    def run(p, at, name, c, i=0):
        work = CUT * 0.004
        if name == "e":
            at += 6 * work + 0.3
            send(p, "x", 8, x_rate, at, p, "p1", c)
        elif name == "z0" and p == 0:
            for j in range(3):
                at += 2 * work + 0.1
                send(p, "in", 2, z_rate, at, 1, "s" + str(j), c)
        elif name in ("z1", "z2"):
            at += 2 * work + 0.1
            send(p, "in", 2, z_rate, at, 1, "s3" if name == "z1" else "s4", c)
        elif name == "z3":
            at += 2 * work + 0.1
            send(p, "out", 2, z_rate, at, 0, "s3", c)
        elif name == "f":
            at += 1.3 * work + 0.1
            send(p, "b", 1, b_rate, at, p, "p3", c)
        elif name == "g":
            at += 4 * work + 0.2
            send(p, "b", 1, b_rate, at, p, "a3", c)
        elif name == "q":
            at += 0.1
            if p == 0:
                send(p, "in", 2, z_rate, at, 1, "n0", c)
            else:
                send(p, "out", 2, z_rate, at, 0, "n0", c)
                send(p, "in", 2, z_rate, at, 1, "n1", c)
        elif name == "i":
            at += 0.3
            if p == 1 and i == 0:
                send(p, "in", 2, z_rate, at, 1, "n2", c)
            elif p == 1:
                send(p, "out", 2, z_rate, at, 0, "n" + str(i), c)
            if i != 1:
                send(p, "x", 4, x_rate, at, p, "a1" if i else "a1 first", c)
        else:
            at += 0.3
            if name == "k":
                send(p, "d", 8, pair_rate, at, p, "a0", c)
        return at

    both = ("l", "e", "z0", "f", "g", "h", "q", "r", "k", "w")
    left = [[(name, c) for c in range(n) for name in both] + [("i", c, i) for c in range(n) for i in range(3)] for _ in range(2)]
    left[1] += [(name, c) for c in range(n) for name in ("z1", "z2", "z3")]
    order = [[], []]
    while left[0] or left[1]:
        best = None
        for p in range(2):
            for one in left[p]:
                times = after(p, *one)
                if None not in times:
                    key = (max(now[p], *times), rank[one[0]], one[1], p, one)
                    best = key if best is None or key < best else best
        at, _, _, p, one = best
        left[p].remove(one)
        now[p] = done[p][one] = run(p, at, *one)
        order[p].append(one)
    return order


def kernel(*refs):
    g, w, m, v = (refs[i : i + 3] for i in (0, 3, 6, 9))
    out, r0, (r1, po, ph, mb, vb) = refs[12:15], refs[15:18], refs[18:23]
    t0, r2, r3, wb = refs[23:27]
    p0s, p0r, lo, lk, lw, lm, p1s, p1r, ks, zr, p3r, a3s, a3r, gs, gr, a1s, a1r, a0s, a0r, lp, credit = refs[27:]
    todo = chunks()
    n = len(todo)

    me = lax.axis_index("dp")
    core, z, y, x = me % 2, me // 2 % 4, me // 8 % 2, me // 16
    a, b = x * (1 - core) + y * core, y * (1 - core) + x * core
    sa, sb = 2 - core, 1 + core
    far = z // 2
    turn = 1 - 2 * far
    here = z * turn + 3 * far
    partner = me + 1 - 2 * core
    beside_a = ((1 - a) * sa + b * sb) * 8 + z * 2 + core
    beside_b = (a * sa + (1 - b) * sb) * 8 + z * 2 + core
    inward, outward = me + 2 * turn, me - 2 * turn

    own_xy, other_xy = [a * sa, a * sa + sb], [(1 - a) * sa, (1 - a) * sa + sb]
    line = [t * turn + 3 * far for t in range(4)]
    halves = [pl.ds(2 * far, 2), pl.ds(2 * far + 2 * turn, 2)]
    not_core, not_b, state_xy = 1 - core, 1 - b, x * 2 + y

    def remote(src, dst, send, recv, device):
        return pltpu.make_async_remote_copy(
            src_ref=src, dst_ref=dst, send_sem=send, recv_sem=recv, device_id={"dp": device}, device_id_type=pl.DeviceIdType.MESH
        )

    def await_(ref, sem):
        pltpu.make_async_copy(ref, ref, sem).wait()

    def part(c):
        return pl.ds(todo[c][2], CUT)

    def kept(c, j, t):
        return ph.at[2 * (c % SLOTS), t, 2 + j]

    def kept_r0(c, j, t):
        return ph.at[2 * (c % SLOTS) + 1, t, 2 + j]

    def piece(c, t):
        return ph.at[2 * (c % SLOTS), t, pl.ds(2, 2)]

    def slot(c, i):
        return ph.at[c, i, pl.ds(0, 2)] if i < 4 else r2.at[c]

    def total(i, terms):
        value = terms[0][i].astype(F32)
        for term in terms[1:]:
            value = value + term[i].astype(F32)
        return value.astype(BF16)

    def add(dst, *terms):
        @pl.loop(0, CUT // GROUP)
        def _(i):
            at = pl.ds(i * GROUP, GROUP)
            dst[at] = total(at, terms)

    def p0(c):
        k, l, _ = todo[c]
        return remote(g[k].at[l, :, :, not_core, part(c)], r0[k].at[l, :, :, part(c)], p0s.at[c], p0r.at[c], partner)

    def load_out(c):
        k, l, _ = todo[c]
        return [pltpu.make_async_copy(g[k].at[l, other_xy[j], :, core, part(c)], po.at[c, j], lo.at[c]) for j in range(2)]

    def load_out_r0(c):
        k, l, _ = todo[c]
        return [pltpu.make_async_copy(r0[k].at[l, other_xy[j], :, part(c)], t0.at[c % 3, j], lo.at[c]) for j in range(2)]

    def load_kept(c):
        k, l, _ = todo[c]
        s = c % SLOTS
        return [pltpu.make_async_copy(g[k].at[l, own_xy[j], :, core, part(c)], ph.at[2 * s, :, 2 + j], lk.at[s]) for j in range(2)] + [
            pltpu.make_async_copy(r0[k].at[l, own_xy[j], :, part(c)], ph.at[2 * s + 1, :, 2 + j], lk.at[s]) for j in range(2)
        ]

    def load_state(c):
        k, l, _ = todo[c]
        return [
            pltpu.make_async_copy(w[k].at[l, state_xy, z, core, part(c)], wb.at[c], lw.at[c]),
            pltpu.make_async_copy(m[k].at[l, part(c)], mb.at[c], lm.at[c]),
            pltpu.make_async_copy(v[k].at[l, part(c)], vb.at[c], lm.at[c]),
        ]

    def p1(c):
        return remote(po.at[c], r1.at[c], p1s.at[c], p1r.at[c], beside_a)

    def zsend(c, t, i, device):
        return remote(piece(c, line[t]), slot(c, i), ks.at[c], zr.at[c, i], device)

    def p3(c):
        return remote(kept(c, not_b, z), r3.at[c], ks.at[c], p3r.at[c], beside_b)

    def a3(c):
        return remote(r1.at[c, b, z], r1.at[c, b, z], a3s.at[c], a3r.at[c], beside_b)

    def gsend(c, t, i, device):
        where = r1.at[c, :, line[t]]
        return remote(where, where, gs.at[c], gr.at[c, i], device)

    def a1(c, half):
        at = halves[half]
        return remote(r1.at[c, :, at], po.at[c, :, at], a1s.at[c], a1r.at[c], beside_a)

    def a0(c, mine):
        k, l, _ = todo[c]
        src = r1 if mine else po
        return [
            remote(src.at[c, j], out[k].at[l, (own_xy if mine else other_xy)[j], :, part(c)], a0s.at[c], a0r.at[c], partner) for j in range(2)
        ]

    def sum_piece(c, t, *slots):
        t = line[t]

        @pl.loop(0, 2)
        def _(j):
            add(kept(c, j, t), kept(c, j, t), kept_r0(c, j, t), r1.at[c, j, t], *(slot(c, i).at[j] for i in slots))

    def steps(end):
        freed, ready = set(range(SLOTS)), set()

        def maybe_load(c):
            if c in freed and c in ready:
                for one in load_kept(c):
                    one.start()

        last = (3,) if end else (2, 4)

        def step_l(c):
            await_(r0[todo[c][0]].at[todo[c][1], :, :, part(c)], p0r.at[c])
            for one in load_out_r0(c):
                one.start()
            ready.add(c)
            maybe_load(c)

        def step_e(c):
            await_(t0.at[:2], lo.at[c])

            for j in range(2):

                @pl.loop(0, 4)
                def _(t, j=j):
                    add(po.at[c, j, t], po.at[c, j, t], t0.at[c % 3, j, t])

            p1(c).start()

        def step_z0(c):
            await_(t0.at[:2], lk.at[c % SLOTS])
            await_(r1.at[c], p1r.at[c])
            await_(po.at[c], p1s.at[c])
            pl.semaphore_signal(credit.at[c], inc=1, device_id={"dp": beside_a}, device_id_type=pl.DeviceIdType.MESH)
            if end:
                for i, t in enumerate((3, 2, 1)):
                    sum_piece(c, t)
                    zsend(c, t, i, inward).start()

        def step_z1(c):
            await_(slot(c, 0), zr.at[c, 0])
            sum_piece(c, 3, 0)
            zsend(c, 3, 3, inward).start()

        def step_z2(c):
            await_(slot(c, 1), zr.at[c, 1])
            sum_piece(c, 2, 1)
            zsend(c, 2, 4, inward).start()

        def step_z3(c):
            await_(slot(c, 3), zr.at[c, 3])
            sum_piece(c, 0, 3)
            zsend(c, 0, 3, outward).start()

        def own_terms(c, j):
            return [kept(c, j, z), kept_r0(c, j, z), r1.at[c, j, z], *(slot(c, i).at[j] for i in last)]

        def step_f(c):
            for i in last:
                await_(slot(c, i), zr.at[c, i])
            add(kept(c, not_b, z), *own_terms(c, not_b))
            p3(c).start()

        def step_g(c):
            await_(r3.at[c], p3r.at[c])
            await_(wb.at[c], lw.at[c])
            await_(mb.at[:2], lm.at[c])

            @pl.loop(0, CUT // GROUP)
            def _(i):
                at = pl.ds(i * GROUP, GROUP)
                grad = total(at, [*own_terms(c, b), r3.at[c]]).astype(F32)
                one_m = 0.9 * mb[c, at] + 0.1 * grad
                one_v = 0.95 * vb[c, at] + 0.05 * grad * grad
                one_w = wb[c, at].astype(F32)
                mb[c, at] = one_m
                vb[c, at] = one_v
                r1[c, b, z, at] = (one_w - 0.02 * (one_m * lax.rsqrt(one_v + 1e-8) + 0.1 * one_w)).astype(BF16)

            a3(c).start()

        def step_h(c):
            await_(r1.at[c, not_b, z], a3r.at[c])

        def step_q(c):
            if end:
                gsend(c, 0, 0, inward).start()
            else:
                gsend(c, 1, 0, outward).start()
                gsend(c, 1, 1, inward).start()

        def step_r(c):
            await_(r3.at[:7], ks.at[c])
            freed.add(c + SLOTS)
            maybe_load(c + SLOTS)

        def step_i(c, i):
            t = i + 1 if end else (0, 2, 3)[i]
            await_(r1.at[c, :, line[t]], gr.at[c, i])
            if not end and i == 0:
                gsend(c, 0, 2, inward).start()
            elif not end:
                gsend(c, t, i, outward).start()
            if i == 0:
                pl.semaphore_wait(credit.at[c], 1)
                a1(c, 0).start()
            elif i == 2:
                a1(c, 1).start()
                for one in a0(c, True):
                    one.start()

        def step_k(c):
            await_(r1.at[c], a1r.at[c])
            for one in a0(c, False):
                one.start()

        def step_w(c):
            k, l, _ = todo[c]
            await_(ph.at[c], a0r.at[c])
            pltpu.make_async_copy(out[k].at[l, :, :, part(c)], ph.at[c], lp.at[c]).start()

        return dict(
            l=step_l, e=step_e, z0=step_z0, z1=step_z1, z2=step_z2, z3=step_z3, f=step_f,
            g=step_g, h=step_h, q=step_q, r=step_r, i=step_i, k=step_k, w=step_w,
        )

    for c in range(n):
        p0(c).start()
        for one in load_out(c):
            one.start()
    for c in range(n):
        for one in load_state(c):
            one.start()

    order = plan(n)
    for where in range(2):

        @pl.when(here == where)
        def _():
            take = steps(where == 0)
            for name, *args in order[where]:
                take[name](*args)
            for c in range(n):
                await_(r3.at[: (2, 10)[where]], gs.at[c])

    for c in range(n):
        await_(ph.at[c], lp.at[c])
        await_(ph.at[c], a0s.at[c])
        await_(ph.at[c], p0s.at[c])
        await_(r1.at[c], a1s.at[c])
        await_(r3.at[c], a3s.at[c])


def finish(*refs):
    r1, po, ph, mb, vb = refs[:5]
    new_w, new_m, new_v = (refs[i : i + 3] for i in (5, 8, 11))
    here, there, beside, state = refs[14:]
    me = lax.axis_index("dp")
    core, y, x = me % 2, me // 8 % 2, me // 16
    a = x * (1 - core) + y * core
    sa, sb = 2 - core, 1 + core
    copies = []
    for c, (k, l, o) in enumerate(chunks()):
        at = pl.ds(o, CUT)
        for j in range(2):
            copies.append(pltpu.make_async_copy(r1.at[c, j], new_w[k].at[l, a * sa + j * sb, :, core, at], here.at[c, j]))
            copies.append(pltpu.make_async_copy(po.at[c, j], new_w[k].at[l, (1 - a) * sa + j * sb, :, core, at], there.at[c, j]))
        copies.append(pltpu.make_async_copy(ph.at[c], new_w[k].at[l, :, :, 1 - core, at], beside.at[c]))
        copies.append(pltpu.make_async_copy(mb.at[c], new_m[k].at[l, at], state.at[c, 0]))
        copies.append(pltpu.make_async_copy(vb.at[c], new_v[k].at[l, at], state.at[c, 1]))
    for one in copies:
        one.start()
    for one in copies:
        one.wait()


def solution(mesh):
    shapes = ((40, 3072), (40, 3072), (96, 1280))
    n = len(chunks())
    any_ = pl.BlockSpec(memory_space=pl.ANY)

    def step(*arrays):
        g, w, m, v = (arrays[i : i + 3] for i in (0, 3, 6, 9))
        g = [tiled(one[0], (4, 4, 2), *s) for one, s in zip(g, shapes, strict=True)]
        w = [tiled(one, (4, 4, 2), *s) for one, s in zip(w, shapes, strict=True)]
        m = [tiled(one, (), *s) for one, s in zip(m, shapes, strict=True)]
        v = [tiled(one, (), *s) for one, s in zip(v, shapes, strict=True)]
        dma = lambda *shape: pltpu.SemaphoreType.DMA(shape)
        vmem = lambda *shape, dtype=BF16: pltpu.VMEM((*shape, 8, 128), dtype)
        shape = lambda *shape, dtype=BF16: jax.ShapeDtypeStruct((*shape, 8, 128), dtype)
        on_chip, off_chip = pl.BlockSpec(memory_space=pltpu.VMEM), pl.BlockSpec(memory_space=pltpu.HBM)
        keep = pltpu.with_memory_space_constraint
        *_, r1, po, ph, mb, vb = pl.pallas_call(
            kernel,
            out_shape=[pltpu.HBM((2, 4, 4, TILES, 8, 128), BF16)] * 6
            + [vmem(n, 2, 4, CUT), vmem(n, 2, 4, CUT), vmem(n, 4, 4, CUT), vmem(n, CUT, dtype=F32), vmem(n, CUT, dtype=F32)],
            in_specs=[any_] * 12,
            out_specs=[off_chip] * 6 + [on_chip] * 5,
            scratch_shapes=[
                vmem(3, 2, 4, CUT),
                vmem(n, 2, CUT),
                vmem(n, CUT),
                vmem(n, CUT),
                *(dma(n), dma(n), dma(n), dma(SLOTS), dma(n), dma(n)),
                *(dma(n), dma(n), dma(n), dma(n, 5), dma(n), dma(n), dma(n)),
                *(dma(n), dma(n, 3), dma(n), dma(n), dma(n), dma(n), dma(n)),
                pltpu.SemaphoreType.REGULAR((n,)),
            ],
            compiler_params=pltpu.CompilerParams(has_side_effects=True, vmem_limit_bytes=LIMIT),
        )(*g, *w, *m, *v)
        new = pl.pallas_call(
            finish,
            out_shape=[shape(2, 4, 4, 2, TILES)] * 3 + [shape(2, TILES, dtype=F32)] * 6,
            in_specs=[on_chip] * 5,
            out_specs=[any_] * 9,
            scratch_shapes=[dma(n, 2), dma(n, 2), dma(n), dma(n, 2)],
            compiler_params=pltpu.CompilerParams(vmem_limit_bytes=LIMIT),
        )(*(keep(one, pltpu.VMEM) for one in (r1, po, ph, mb, vb)))
        shape_of = lambda i: shapes[i % 3]
        return tuple(untiled(one, *shape_of(i)) for i, one in enumerate(new))

    all_of, cut = P(None, None, None), P(None, "dp", None)
    return jax.shard_map(
        step,
        mesh=mesh,
        in_specs=(P(("rep", "dp"), None, None, None),) * 3 + (all_of,) * 3 + (cut,) * 6,
        out_specs=(P("rep", None, None),) * 3 + (P("rep", "dp", None),) * 6,
        check_vma=False,
    )
```

```python
import functools

import jax
import jax.numpy as jnp
from jax import lax
from jax.experimental import pallas as pl
from jax.experimental.pallas import tpu as pltpu
from jax.sharding import PartitionSpec as P

TILES = 120
CUT = 40
GROUP = 20
SLOTS = 9
HOLD = 6
LIMIT = 9 << 20
F32, BF16 = jnp.float32, jnp.bfloat16


def tiled(a, lead, rows, columns):
    a = a.reshape(2, *lead, rows // 8, 8, columns // 128, 128)
    return jnp.swapaxes(a, a.ndim - 3, a.ndim - 2).reshape(2, *lead, TILES, 8, 128)


def untiled(a, rows, columns):
    n = a.size // (2 * rows * columns)
    a = a.reshape(2, n, rows // 8, columns // 128, 8, 128)
    return jnp.swapaxes(a, 3, 4).reshape(2, n * rows, columns)


def chunks():
    return [(k, l, o) for k in range(3) for l in range(2) for o in range(0, TILES, CUT)]


def plan(n):
    tile = 2048e-3
    hop, z_rate, x_rate, b_rate, pair_rate = 2.0, 46.6e3, 80e3, 30e3, 540e3
    rank = dict(z1=0, z2=0, z3=0, z0=1, f=2, g=3, e=4, l=4, h=5, q=5.5, i=6, r=7, k=8, w=9)
    free, arrived, sent, now = {}, {}, {}, [0.0, 0.0]
    done = [{}, {}]
    pair = 4.0
    for c in range(n):
        pair += 16 * CUT * tile / pair_rate * 1e3
        arrived[0, "p0", c] = arrived[1, "p0", c] = pair + hop

    def send(p, link, blocks, rate, at, to, *name):
        start = max(at + 0.3, free.get((p, link), 0.0))
        end = start + blocks * CUT * tile / rate * 1e3 + (0.4 if link == "x" else 0.0)
        free[p, link] = end
        arrived[(to, *name)] = end + hop
        sent[(p, link, *name)] = end + hop

    def after(p, name, c, i=0):
        past = lambda *one, plus=0.0: None if one not in done[p] else done[p][one] + plus
        come = lambda *one: arrived.get((p, *one))
        if name == "l":
            return [come("p0", c)] + ([past("l", c - 1)] if c else []) + ([past("e", c - 3)] if c >= 3 else [])
        if name == "e":
            return [past("l", c, plus=1.5)]
        if name == "z0":
            return [come("p1", c), past("l", c, plus=1.5)] + ([past("r", c - SLOTS, plus=1.5)] if c >= SLOTS else [])
        if name in ("z1", "z2", "z3"):
            return [past("z0", c), come("s" + str((0, 1, 3)[int(name[1]) - 1]), c)]
        if name == "f":
            if p == 0:
                return [past("z0", c), come("s3", c)]
            return [past("z1", c), past("z2", c), past("z3", c), come("s2", c), come("s4", c)]
        if name == "g":
            return [past("f", c), come("p3", c)]
        if name == "h":
            return [past("g", c), come("a3", c)]
        if name == "q":
            return [past("h", c)] + ([past("z0", min(n - 1, c + HOLD))] if p == 0 else [])
        if name == "r":
            if p == 0:
                sends = [sent.get((p, "in", "s" + str(j), c)) for j in range(3)]
            else:
                sends = [sent.get((p, *one, c)) for one in (("in", "s3"), ("in", "s4"), ("out", "s3"))]
            return [past("g", c), sent.get((p, "b", "p3", c)), *sends]
        if name == "i":
            return [past("q", c), come("n" + str(i), c)] + ([past("i", c, i - 1)] if i else [])
        if name == "k":
            return [past("i", c, 2), come("a1", c)]
        return [past("k", c), come("a0", c)] + [past("r", j) for j in range(n)]

    def run(p, at, name, c, i=0):
        work = CUT * 0.004
        if name == "e":
            at += 6 * work + 0.3
            send(p, "x", 8, x_rate, at, p, "p1", c)
        elif name == "z0" and p == 0:
            for j in range(3):
                at += 2 * work + 0.1
                send(p, "in", 2, z_rate, at, 1, "s" + str(j), c)
        elif name in ("z1", "z2"):
            at += 2 * work + 0.1
            send(p, "in", 2, z_rate, at, 1, "s3" if name == "z1" else "s4", c)
        elif name == "z3":
            at += 2 * work + 0.1
            send(p, "out", 2, z_rate, at, 0, "s3", c)
        elif name == "f":
            at += 1.3 * work + 0.1
            send(p, "b", 1, b_rate, at, p, "p3", c)
        elif name == "g":
            at += 4 * work + 0.2
            send(p, "b", 1, b_rate, at, p, "a3", c)
        elif name == "q":
            at += 0.1
            if p == 0:
                send(p, "in", 2, z_rate, at, 1, "n0", c)
            else:
                send(p, "out", 2, z_rate, at, 0, "n0", c)
                send(p, "in", 2, z_rate, at, 1, "n1", c)
        elif name == "i":
            at += 0.3
            if p == 1 and i == 0:
                send(p, "in", 2, z_rate, at, 1, "n2", c)
            elif p == 1:
                send(p, "out", 2, z_rate, at, 0, "n" + str(i), c)
            if i != 1:
                send(p, "x", 4, x_rate, at, p, "a1" if i else "a1 first", c)
        else:
            at += 0.3
            if name == "k":
                send(p, "d", 8, pair_rate, at, p, "a0", c)
        return at

    both = ("l", "e", "z0", "f", "g", "h", "q", "r", "k", "w")
    left = [[(name, c) for c in range(n) for name in both] + [("i", c, i) for c in range(n) for i in range(3)] for _ in range(2)]
    left[1] += [(name, c) for c in range(n) for name in ("z1", "z2", "z3")]
    order = [[], []]
    while left[0] or left[1]:
        best = None
        for p in range(2):
            for one in left[p]:
                times = after(p, *one)
                if None not in times:
                    key = (max(now[p], *times), rank[one[0]], one[1], p, one)
                    best = key if best is None or key < best else best
        at, _, _, p, one = best
        left[p].remove(one)
        now[p] = done[p][one] = run(p, at, *one)
        order[p].append(one)
    return order


def kernel(*refs):
    g, w, m, v = (refs[i : i + 3] for i in (0, 3, 6, 9))
    out, r0, (r1, po, ph, mb, vb) = refs[12:15], refs[15:18], refs[18:23]
    t0, r2, r3, wb = refs[23:27]
    p0s, p0r, lo, lk, lw, lm, p1s, p1r, ks, zr, p3r, a3s, a3r, gs, gr, a1s, a1r, a0s, a0r, lp, credit = refs[27:]
    todo = chunks()
    n = len(todo)

    me = lax.axis_index("dp")
    core, z, y, x = me % 2, me // 2 % 4, me // 8 % 2, me // 16
    a, b = x * (1 - core) + y * core, y * (1 - core) + x * core
    sa, sb = 2 - core, 1 + core
    far = z // 2
    turn = 1 - 2 * far
    here = z * turn + 3 * far
    partner = me + 1 - 2 * core
    beside_a = ((1 - a) * sa + b * sb) * 8 + z * 2 + core
    beside_b = (a * sa + (1 - b) * sb) * 8 + z * 2 + core
    inward, outward = me + 2 * turn, me - 2 * turn

    own_xy, other_xy = [a * sa, a * sa + sb], [(1 - a) * sa, (1 - a) * sa + sb]
    line = [t * turn + 3 * far for t in range(4)]
    halves = [pl.ds(2 * far, 2), pl.ds(2 * far + 2 * turn, 2)]
    not_core, not_b, state_xy = 1 - core, 1 - b, x * 2 + y

    def remote(src, dst, send, recv, device):
        return pltpu.make_async_remote_copy(
            src_ref=src, dst_ref=dst, send_sem=send, recv_sem=recv, device_id={"dp": device}, device_id_type=pl.DeviceIdType.MESH
        )

    def await_(ref, sem):
        pltpu.make_async_copy(ref, ref, sem).wait()

    def part(c):
        return pl.ds(todo[c][2], CUT)

    def kept(c, j, t):
        return ph.at[2 * (c % SLOTS), t, 2 + j]

    def kept_r0(c, j, t):
        return ph.at[2 * (c % SLOTS) + 1, t, 2 + j]

    def piece(c, t):
        return ph.at[2 * (c % SLOTS), t, pl.ds(2, 2)]

    def slot(c, i):
        return ph.at[c, i, pl.ds(0, 2)] if i < 4 else r2.at[c]

    def total(i, terms):
        value = terms[0][i].astype(F32)
        for term in terms[1:]:
            value = value + term[i].astype(F32)
        return value.astype(BF16)

    def add(dst, *terms):
        @pl.loop(0, CUT // GROUP)
        def _(i):
            at = pl.ds(i * GROUP, GROUP)
            dst[at] = total(at, terms)

    def p0(c):
        k, l, _ = todo[c]
        return remote(g[k].at[l, :, :, not_core, part(c)], r0[k].at[l, :, :, part(c)], p0s.at[c], p0r.at[c], partner)

    def load_out(c):
        k, l, _ = todo[c]
        return [pltpu.make_async_copy(g[k].at[l, other_xy[j], :, core, part(c)], po.at[c, j], lo.at[c]) for j in range(2)]

    def load_out_r0(c):
        k, l, _ = todo[c]
        return [pltpu.make_async_copy(r0[k].at[l, other_xy[j], :, part(c)], t0.at[c % 3, j], lo.at[c]) for j in range(2)]

    def load_kept(c):
        k, l, _ = todo[c]
        s = c % SLOTS
        return [pltpu.make_async_copy(g[k].at[l, own_xy[j], :, core, part(c)], ph.at[2 * s, :, 2 + j], lk.at[s]) for j in range(2)] + [
            pltpu.make_async_copy(r0[k].at[l, own_xy[j], :, part(c)], ph.at[2 * s + 1, :, 2 + j], lk.at[s]) for j in range(2)
        ]

    def load_state(c):
        k, l, _ = todo[c]
        return [
            pltpu.make_async_copy(w[k].at[l, state_xy, z, core, part(c)], wb.at[c], lw.at[c]),
            pltpu.make_async_copy(m[k].at[l, part(c)], mb.at[c], lm.at[c]),
            pltpu.make_async_copy(v[k].at[l, part(c)], vb.at[c], lm.at[c]),
        ]

    def p1(c):
        return remote(po.at[c], r1.at[c], p1s.at[c], p1r.at[c], beside_a)

    def zsend(c, t, i, device):
        return remote(piece(c, line[t]), slot(c, i), ks.at[c], zr.at[c, i], device)

    def p3(c):
        return remote(kept(c, not_b, z), r3.at[c], ks.at[c], p3r.at[c], beside_b)

    def a3(c):
        return remote(r1.at[c, b, z], r1.at[c, b, z], a3s.at[c], a3r.at[c], beside_b)

    def gsend(c, t, i, device):
        where = r1.at[c, :, line[t]]
        return remote(where, where, gs.at[c], gr.at[c, i], device)

    def a1(c, half):
        at = halves[half]
        return remote(r1.at[c, :, at], po.at[c, :, at], a1s.at[c], a1r.at[c], beside_a)

    def a0(c, mine):
        k, l, _ = todo[c]
        src = r1 if mine else po
        return [
            remote(src.at[c, j], out[k].at[l, (own_xy if mine else other_xy)[j], :, part(c)], a0s.at[c], a0r.at[c], partner) for j in range(2)
        ]

    def sum_piece(c, t, *slots):
        t = line[t]

        @pl.loop(0, 2)
        def _(j):
            add(kept(c, j, t), kept(c, j, t), kept_r0(c, j, t), r1.at[c, j, t], *(slot(c, i).at[j] for i in slots))

    def steps(end):
        freed, ready = set(range(SLOTS)), set()

        def maybe_load(c):
            if c in freed and c in ready:
                for one in load_kept(c):
                    one.start()

        last = (3,) if end else (2, 4)

        def step_l(c):
            await_(r0[todo[c][0]].at[todo[c][1], :, :, part(c)], p0r.at[c])
            for one in load_out_r0(c):
                one.start()
            ready.add(c)
            maybe_load(c)

        def step_e(c):
            await_(t0.at[:2], lo.at[c])

            for j in range(2):

                @pl.loop(0, 4)
                def _(t, j=j):
                    add(po.at[c, j, t], po.at[c, j, t], t0.at[c % 3, j, t])

            p1(c).start()

        def step_z0(c):
            await_(t0.at[:2], lk.at[c % SLOTS])
            await_(r1.at[c], p1r.at[c])
            await_(po.at[c], p1s.at[c])
            pl.semaphore_signal(credit.at[c], inc=1, device_id={"dp": beside_a}, device_id_type=pl.DeviceIdType.MESH)
            if end:
                for i, t in enumerate((3, 2, 1)):
                    sum_piece(c, t)
                    zsend(c, t, i, inward).start()

        def step_z1(c):
            await_(slot(c, 0), zr.at[c, 0])
            sum_piece(c, 3, 0)
            zsend(c, 3, 3, inward).start()

        def step_z2(c):
            await_(slot(c, 1), zr.at[c, 1])
            sum_piece(c, 2, 1)
            zsend(c, 2, 4, inward).start()

        def step_z3(c):
            await_(slot(c, 3), zr.at[c, 3])
            sum_piece(c, 0, 3)
            zsend(c, 0, 3, outward).start()

        def own_terms(c, j):
            return [kept(c, j, z), kept_r0(c, j, z), r1.at[c, j, z], *(slot(c, i).at[j] for i in last)]

        def step_f(c):
            for i in last:
                await_(slot(c, i), zr.at[c, i])
            add(kept(c, not_b, z), *own_terms(c, not_b))
            p3(c).start()

        def step_g(c):
            await_(r3.at[c], p3r.at[c])
            await_(wb.at[c], lw.at[c])
            await_(mb.at[:2], lm.at[c])

            @pl.loop(0, CUT // GROUP)
            def _(i):
                at = pl.ds(i * GROUP, GROUP)
                grad = total(at, [*own_terms(c, b), r3.at[c]]).astype(F32)
                one_m = 0.9 * mb[c, at] + 0.1 * grad
                one_v = 0.95 * vb[c, at] + 0.05 * grad * grad
                one_w = wb[c, at].astype(F32)
                mb[c, at] = one_m
                vb[c, at] = one_v
                r1[c, b, z, at] = (one_w - 0.02 * (one_m * lax.rsqrt(one_v + 1e-8) + 0.1 * one_w)).astype(BF16)

            a3(c).start()

        def step_h(c):
            await_(r1.at[c, not_b, z], a3r.at[c])

        def step_q(c):
            if end:
                gsend(c, 0, 0, inward).start()
            else:
                gsend(c, 1, 0, outward).start()
                gsend(c, 1, 1, inward).start()

        def step_r(c):
            await_(r3.at[:7], ks.at[c])
            freed.add(c + SLOTS)
            maybe_load(c + SLOTS)

        def step_i(c, i):
            t = i + 1 if end else (0, 2, 3)[i]
            await_(r1.at[c, :, line[t]], gr.at[c, i])
            if not end and i == 0:
                gsend(c, 0, 2, inward).start()
            elif not end:
                gsend(c, t, i, outward).start()
            if i == 0:
                pl.semaphore_wait(credit.at[c], 1)
                a1(c, 0).start()
            elif i == 2:
                a1(c, 1).start()
                for one in a0(c, True):
                    one.start()

        def step_k(c):
            await_(r1.at[c], a1r.at[c])
            for one in a0(c, False):
                one.start()

        def step_w(c):
            k, l, _ = todo[c]
            await_(ph.at[c], a0r.at[c])
            pltpu.make_async_copy(out[k].at[l, :, :, part(c)], ph.at[c], lp.at[c]).start()

        return dict(
            l=step_l, e=step_e, z0=step_z0, z1=step_z1, z2=step_z2, z3=step_z3, f=step_f,
            g=step_g, h=step_h, q=step_q, r=step_r, i=step_i, k=step_k, w=step_w,
        )

    for c in range(n):
        p0(c).start()
        for one in load_out(c):
            one.start()
    for c in range(n):
        for one in load_state(c):
            one.start()

    order = plan(n)
    for where in range(2):

        @pl.when(here == where)
        def _():
            take = steps(where == 0)
            for name, *args in order[where]:
                take[name](*args)
            for c in range(n):
                await_(r3.at[: (2, 10)[where]], gs.at[c])

    for c in range(n):
        await_(ph.at[c], lp.at[c])
        await_(ph.at[c], a0s.at[c])
        await_(ph.at[c], p0s.at[c])
        await_(r1.at[c], a1s.at[c])
        await_(r3.at[c], a3s.at[c])


def finish(*refs):
    r1, po, ph, mb, vb = refs[:5]
    new_w, new_m, new_v = (refs[i : i + 3] for i in (5, 8, 11))
    here, there, beside, state = refs[14:]
    me = lax.axis_index("dp")
    core, y, x = me % 2, me // 8 % 2, me // 16
    a = x * (1 - core) + y * core
    sa, sb = 2 - core, 1 + core
    copies = []
    for c, (k, l, o) in enumerate(chunks()):
        at = pl.ds(o, CUT)
        for j in range(2):
            copies.append(pltpu.make_async_copy(r1.at[c, j], new_w[k].at[l, a * sa + j * sb, :, core, at], here.at[c, j]))
            copies.append(pltpu.make_async_copy(po.at[c, j], new_w[k].at[l, (1 - a) * sa + j * sb, :, core, at], there.at[c, j]))
        copies.append(pltpu.make_async_copy(ph.at[c], new_w[k].at[l, :, :, 1 - core, at], beside.at[c]))
        copies.append(pltpu.make_async_copy(mb.at[c], new_m[k].at[l, at], state.at[c, 0]))
        copies.append(pltpu.make_async_copy(vb.at[c], new_v[k].at[l, at], state.at[c, 1]))
    for one in copies:
        one.start()
    for one in copies:
        one.wait()


def solution(mesh):
    shapes = ((40, 3072), (40, 3072), (96, 1280))
    n = len(chunks())
    any_ = pl.BlockSpec(memory_space=pl.ANY)

    def step(*arrays):
        g, w, m, v = (arrays[i : i + 3] for i in (0, 3, 6, 9))
        g = [tiled(one[0], (4, 4, 2), *s) for one, s in zip(g, shapes, strict=True)]
        w = [tiled(one, (4, 4, 2), *s) for one, s in zip(w, shapes, strict=True)]
        m = [tiled(one, (), *s) for one, s in zip(m, shapes, strict=True)]
        v = [tiled(one, (), *s) for one, s in zip(v, shapes, strict=True)]
        dma = lambda *shape: pltpu.SemaphoreType.DMA(shape)
        vmem = lambda *shape, dtype=BF16: pltpu.VMEM((*shape, 8, 128), dtype)
        shape = lambda *shape, dtype=BF16: jax.ShapeDtypeStruct((*shape, 8, 128), dtype)
        on_chip, off_chip = pl.BlockSpec(memory_space=pltpu.VMEM), pl.BlockSpec(memory_space=pltpu.HBM)
        keep = pltpu.with_memory_space_constraint
        *_, r1, po, ph, mb, vb = pl.pallas_call(
            kernel,
            out_shape=[pltpu.HBM((2, 4, 4, TILES, 8, 128), BF16)] * 6
            + [vmem(n, 2, 4, CUT), vmem(n, 2, 4, CUT), vmem(n, 4, 4, CUT), vmem(n, CUT, dtype=F32), vmem(n, CUT, dtype=F32)],
            in_specs=[any_] * 12,
            out_specs=[off_chip] * 6 + [on_chip] * 5,
            scratch_shapes=[
                vmem(3, 2, 4, CUT),
                vmem(n, 2, CUT),
                vmem(n, CUT),
                vmem(n, CUT),
                *(dma(n), dma(n), dma(n), dma(SLOTS), dma(n), dma(n)),
                *(dma(n), dma(n), dma(n), dma(n, 5), dma(n), dma(n), dma(n)),
                *(dma(n), dma(n, 3), dma(n), dma(n), dma(n), dma(n), dma(n)),
                pltpu.SemaphoreType.REGULAR((n,)),
            ],
            compiler_params=pltpu.CompilerParams(has_side_effects=True, vmem_limit_bytes=LIMIT),
        )(*g, *w, *m, *v)
        new = pl.pallas_call(
            finish,
            out_shape=[shape(2, 4, 4, 2, TILES)] * 3 + [shape(2, TILES, dtype=F32)] * 6,
            in_specs=[on_chip] * 5,
            out_specs=[any_] * 9,
            scratch_shapes=[dma(n, 2), dma(n, 2), dma(n), dma(n, 2)],
            compiler_params=pltpu.CompilerParams(vmem_limit_bytes=LIMIT),
        )(*(keep(one, pltpu.VMEM) for one in (r1, po, ph, mb, vb)))
        shape_of = lambda i: shapes[i % 3]
        return tuple(untiled(one, *shape_of(i)) for i, one in enumerate(new))

    all_of, cut = P(None, None, None), P(None, "dp", None)
    return jax.shard_map(
        step,
        mesh=mesh,
        in_specs=(P(("rep", "dp"), None, None, None),) * 3 + (all_of,) * 3 + (cut,) * 6,
        out_specs=(P("rep", None, None),) * 3 + (P("rep", "dp", None),) * 6,
        check_vma=False,
    )
```
